32 devices in a mesh: dp: 16 (over z, y, core), tensor: 2 (over x).
Axes of the slice: x: 2, y: 2, z: 4, core: 2. Of those that a mesh axis runs over, the one named last changes fastest.
Arguments:
- layer_input: bfloat16 [16384, 1024], P(('dp', 'tensor')), may hold values from -6 to 6
- segments: int32 [16384], P('dp'), may hold values from 0 to 127, never falling along the last dimension, each value on 1 to 256 neighbouring positions
- w_qkv: bfloat16 [1024, 3, 1024], P(None, None, 'tensor'), may hold values from -0.1875 to 0.1875
- w_out: bfloat16 [1024, 1024], P('tensor'), may hold values from -2 to 2
- w_up: bfloat16 [1024, 4096], P(None, 'tensor'), may hold values from -0.1875 to 0.1875
- w_down: bfloat16 [4096, 1024], P('tensor'), may hold values from -0.09375 to 0.09375
- norm1_gain: float32 [1024], replicated, may hold values from 0.5 to 1.5
- norm1_bias: float32 [1024], replicated, may hold values from -3 to 3
- norm2_gain: float32 [1024], replicated, may hold values from 0.5 to 1.5
- norm2_bias: float32 [1024], replicated, may hold values from -3 to 3
- out_grad: bfloat16 [16384, 1024], P(('dp', 'tensor')), may hold values from -6 to 6
Outputs:
- output: bfloat16 [16384, 1024], P(('dp', 'tensor'))
- input_grad: bfloat16 [16384, 1024], P(('dp', 'tensor'))
- grad_qkv: float32 [1024, 3, 1024], P(None, None, 'tensor')
- grad_out: float32 [1024, 1024], P('tensor')
- grad_up: float32 [1024, 4096], P(None, 'tensor')
- grad_down: float32 [4096, 1024], P('tensor')
- grad_gain1: float32 [1024], replicated
- grad_bias1: float32 [1024], replicated
- grad_gain2: float32 [1024], replicated
- grad_bias2: float32 [1024], replicated
The draws below stay inside these ranges and needn't reach their ends.
Inputs may be any that keep to these rules, and one draw needn't show every extreme that they name: `segments`: segment ids never fall along the tokens; each protein has 1 to 256 tokens and attends only within its packed row of 512.
All inputs are finite; a program needn't handle non-finite values.
Results may differ from the reference program's by a relative error of at most 0.02.
Values may be sent and summed in bfloat16 or wider, within the bound.
A program may use at most 192 MiB of HBM per device.

```python
import math
import jax
import jax.numpy as jnp
import numpy as np
from jax import lax

D = 1024
HEADS = 16
HEAD_DIM = 64
FF = 4096
ROW_LEN = 512
TOKENS = 16384


def level_of(rng, shape, pieces, smallest, high):
    def one(axis_at, parts):
        steps = jax.random.uniform(jax.random.fold_in(jax.random.fold_in(rng, 6), axis_at), (parts,), jnp.float32, smallest / len(pieces), high / len(pieces))
        return jnp.repeat(jnp.exp(steps), shape[axis_at] // parts).reshape((-1,) + (1,) * (len(shape) - axis_at - 1))

    loudness = one(*pieces[0])
    for cut in pieces[1:]:
        loudness = loudness * one(*cut)
    return loudness


def profile(count, total, most, skew):
    loads = [(1 << 20) // math.isqrt(rank ** skew) + 1 for rank in range(2, count + 1)]
    spare, holding = total - most - (count - 1), [1] * (count - 1)
    while spare > 0:
        free = [i for i in range(count - 1) if holding[i] < most]
        whole, left = sum([loads[i] for i in free]), spare
        for i in free:
            extra = min(most - holding[i], max(1, left * loads[i] // whole), spare)
            holding[i] = holding[i] + extra
            spare = spare - extra
    return np.array([most] + holding)


def ragged(key, amount, total, reach, lean):
    if amount == 2:
        one = jax.random.randint(key, (), max(1, total - reach), min(reach, total - 1) + 1)
        return jnp.stack([one, total - one])
    sizes = jnp.asarray(profile(amount, total, reach, lean), jnp.int32)
    twos = (amount - 1) // 2
    donor, sink = sizes[1:1 + 2 * twos:2], sizes[2:2 + 2 * twos:2]
    margin = jnp.minimum(donor - 1, reach - sink)
    passed = jax.random.randint(jax.random.fold_in(key, 1), (twos,), 0, 1 << 20) % (margin + 1)
    sizes = sizes.at[1:1 + 2 * twos:2].set(donor - passed).at[2:2 + 2 * twos:2].set(sink + passed)
    return sizes[jax.random.permutation(jax.random.fold_in(key, 2), amount)]


def bell_draw(stream_key, shape, deviation, reach, pieces=(), dtype=jnp.bfloat16):
    entries = deviation * jax.random.normal(stream_key, shape, jnp.float32)
    if pieces:
        entries = entries * level_of(stream_key, shape, pieces, -0.22, 0.18)
    return jnp.clip(entries, -reach, reach).astype(dtype)


def setup_inputs(seed: int = 0) -> dict:
    key_of = jax.random.split(jax.random.key(seed), 12)
    layer_input = bell_draw(key_of[0], (TOKENS, D), 1.0, 6.0, ((0, 32),))
    segments = jnp.searchsorted(jnp.cumsum(ragged(key_of[1], TOKENS * 4 // ROW_LEN, TOKENS, ROW_LEN // 2, 1)), jnp.arange(TOKENS), side="right").astype(jnp.int32)
    w_qkv = bell_draw(key_of[2], (D, 3, D), D ** -0.5, 0.1875, ((2, 2),))
    w_out = bell_draw(key_of[3], (D, D), (max(D // 128, 4)) ** -0.5, 2.0, ((0, 2),))
    w_up = bell_draw(key_of[4], (D, FF), D ** -0.5, 0.1875, ((1, 2),))
    w_down = bell_draw(key_of[5], (FF, D), FF ** -0.5, 0.09375, ((0, 2),))
    norm1_gain = jnp.clip(1.0 + 0.1 * jax.random.normal(key_of[6], (D,), jnp.float32), 0.5, 1.5)
    norm1_bias = bell_draw(key_of[7], (D,), 0.5, 3.0, (), jnp.float32)
    norm2_gain = jnp.clip(1.0 + 0.1 * jax.random.normal(key_of[8], (D,), jnp.float32), 0.5, 1.5)
    norm2_bias = bell_draw(key_of[9], (D,), 0.5, 3.0, (), jnp.float32)
    out_grad = bell_draw(key_of[10], (TOKENS, D), 1.0, 6.0, ((0, 32),))
    return {"layer_input": layer_input, "segments": segments, "w_qkv": w_qkv, "w_out": w_out, "w_up": w_up, "w_down": w_down, "norm1_gain": norm1_gain, "norm1_bias": norm1_bias, "norm2_gain": norm2_gain, "norm2_bias": norm2_bias, "out_grad": out_grad}


@jax.custom_vjp
def low(v):
    return lax.optimization_barrier(v.astype(jnp.bfloat16)).astype(jnp.float32)

@jax.custom_vjp
def low_back(v):
    return v

def low_keep(v):
    return (low(v), None)

def low_pass(kept, grad):
    return (grad,)

def back_keep(v):
    return (v, None)

def back_low(kept, grad):
    return (low(grad),)
low.defvjp(low_keep, low_pass)
low_back.defvjp(back_keep, back_low)
EPS = 1e-12
NEG_LARGE = -1e+30
SQRT_HALF = 0.7071067811865476
HIGHEST = lax.Precision.HIGHEST

def gelu_exact(values):
    return 0.5 * values * (1.0 + lax.erf(values * SQRT_HALF))

def layer_norm(values, gain, bias):
    average = lax.optimization_barrier(jnp.mean(values, axis=-1, keepdims=True))
    centred = values - average
    inverse = lax.rsqrt(lax.optimization_barrier(jnp.mean(centred * centred, axis=-1, keepdims=True)) + EPS)
    return centred * inverse * gain + bias

def attend_row(pack):
    block, row_segments = pack
    queries = block[:, 0]
    keys = block[:, 1]
    values = block[:, 2]
    scores = jnp.einsum('qhd,khd->hqk', queries, keys, precision=HIGHEST) * HEAD_DIM ** (-0.5)
    scores = low_back(scores)
    same = row_segments[:, None] == row_segments[None, :]
    scores = jnp.where(same[None], scores, NEG_LARGE)
    top = lax.optimization_barrier(jnp.max(scores, axis=-1, keepdims=True))
    expo = jnp.exp(scores - top)
    probs = expo / lax.optimization_barrier(jnp.sum(expo, axis=-1, keepdims=True))
    mixed = jnp.einsum('hqk,khd->qhd', low(probs), values, precision=HIGHEST)
    return mixed.reshape(ROW_LEN, D)

def reference(layer_input, segments, w_qkv, w_out, w_up, w_down, norm1_gain, norm1_bias, norm2_gain, norm2_bias, out_grad):
    row_count = TOKENS // ROW_LEN
    row_segments = segments.reshape(row_count, ROW_LEN)

    def layer(inputs, qkv_w, out_w, up_w, down_w, gain1, bias1, gain2, bias2):
        joined = jnp.einsum('td,dsc->tsc', inputs, qkv_w, precision=HIGHEST)
        joined = low(low_back(joined))
        shaped = joined.reshape(row_count, ROW_LEN, 3, HEADS, HEAD_DIM)
        mixed = lax.map(jax.checkpoint(attend_row), (shaped, row_segments))
        mixed = low(low_back(mixed.reshape(TOKENS, D)))
        attn_out = low_back(jnp.dot(mixed, out_w, precision=HIGHEST))
        hidden = layer_norm(inputs + attn_out, gain1, bias1)
        hidden_low = low(hidden)
        upper = low_back(jnp.dot(hidden_low, up_w, precision=HIGHEST))
        active = low(gelu_exact(upper))
        ffn_out = low_back(jnp.dot(active, down_w, precision=HIGHEST))
        return layer_norm(hidden + ffn_out, gain2, bias2)
    primals = (layer_input.astype(jnp.float32), w_qkv.astype(jnp.float32), w_out.astype(jnp.float32), w_up.astype(jnp.float32), w_down.astype(jnp.float32), norm1_gain.astype(jnp.float32), norm1_bias.astype(jnp.float32), norm2_gain.astype(jnp.float32), norm2_bias.astype(jnp.float32))
    result, pullback = jax.vjp(layer, *primals)
    grads = pullback(out_grad.astype(jnp.float32))
    return (result.astype(jnp.bfloat16), grads[0].astype(jnp.bfloat16), grads[1], grads[2], grads[3], grads[4], grads[5], grads[6], grads[7], grads[8])
```

```python
import jax
import jax.numpy as jnp
from jax import lax
from jax.sharding import PartitionSpec as P

HEAD_DIM = 64
ROW_LEN = 512


EPS = 1e-12
NEG_LARGE = -1e30
SQRT_HALF = 0.7071067811865476
INV_ROOT_TWO_PI = 0.3989422804014327


def gelu_exact(values):
    return 0.5 * values * (1.0 + lax.erf(values * SQRT_HALF))


def gelu_slope(values):
    return (
        0.5 * (1.0 + lax.erf(values * SQRT_HALF))
        + values * jnp.exp(-0.5 * values * values) * INV_ROOT_TWO_PI
    )


def layer_norm(values, gain, bias):
    average = jnp.mean(values, axis=-1, keepdims=True)
    centred = values - average
    inverse = lax.rsqrt(jnp.mean(centred * centred, axis=-1, keepdims=True) + EPS)
    normed = centred * inverse
    return (normed * gain + bias, normed, inverse)


def norm_back(grad, normed, inverse, gain):
    scaled = grad * gain
    return inverse * (
        scaled
        - jnp.mean(scaled, axis=-1, keepdims=True)
        - normed * jnp.mean(scaled * normed, axis=-1, keepdims=True)
    )


def masked_scores(queries, keys, row_segments, factor):
    scores = jnp.einsum("qhd,khd->hqk", queries, keys, preferred_element_type=jnp.float32) * factor
    same = row_segments[:, None] == row_segments[None, :]
    return jnp.where(same[None], scores, NEG_LARGE)


def contract_rows(left, right):
    return lax.dot_general(
        left, right, (((0,), (0,)), ((), ())), preferred_element_type=jnp.float32
    )


def contract_cols(left, right):
    return lax.dot_general(
        left, right, (((1,), (1,)), ((), ())), preferred_element_type=jnp.float32
    )


def _pair_swap(values):
    return lax.ppermute(values, "tensor", [(0, 1), (1, 0)])


def gather_group(values, pair):
    if pair:
        return jnp.concatenate([values, _pair_swap(values)], axis=0)
    return lax.all_gather(values, "tensor", axis=0, tiled=True)


def scatter_group(values, pair):
    if pair:
        rows = values.shape[0] // 2
        own = values[:rows].astype(jnp.float32)
        other = _pair_swap(values[rows:].astype(jnp.bfloat16))
        return own + other.astype(jnp.float32)
    return lax.psum_scatter(
        values.astype(jnp.bfloat16), "tensor", scatter_dimension=0, tiled=True
    ).astype(jnp.float32)


def body(
    layer_input,
    segments,
    w_qkv,
    w_out,
    w_up,
    w_down,
    norm1_gain,
    norm1_bias,
    norm2_gain,
    norm2_bias,
    out_grad,
):
    head_width = HEAD_DIM
    row_length = ROW_LEN
    factor = head_width ** (-0.5)
    qkv_use, out_use = (w_qkv, w_out)
    pair = lax.axis_size("tensor") == 2
    source = gather_group(layer_input, pair)
    local_width = qkv_use.shape[2]
    local_heads = local_width // head_width
    group_rows = source.shape[0]
    blocks = group_rows // row_length
    joined = jnp.einsum("td,dsc->tsc", source, qkv_use, preferred_element_type=jnp.float32).astype(
        jnp.bfloat16
    )
    joined_blocks = joined.reshape(blocks, row_length, 3, local_heads, head_width)
    if pair:
        me = lax.axis_index("tensor")
        own_seg = lax.dynamic_slice_in_dim(segments, me * row_length, row_length)
        other_seg = lax.dynamic_slice_in_dim(segments, (1 - me) * row_length, row_length)
        segments = jnp.concatenate([own_seg, other_seg])
    segment_blocks = segments.reshape(blocks, row_length)

    def attend(pack):
        block, row_segments = pack
        scores = masked_scores(block[:, 0], block[:, 1], row_segments, factor)
        top = jnp.max(scores, axis=-1, keepdims=True)
        expo = jnp.exp(scores - top)
        total = jnp.sum(expo, axis=-1, keepdims=True)
        probs = (expo / total).astype(jnp.bfloat16)
        mixed = jnp.einsum("hqk,khd->qhd", probs, block[:, 2], preferred_element_type=jnp.float32)
        return (
            mixed.reshape(row_length, local_width).astype(jnp.bfloat16),
            (top + jnp.log(total))[..., 0],
        )

    attended, log_totals = lax.map(attend, (joined_blocks, segment_blocks))
    attended = attended.reshape(group_rows, local_width)
    attn_out = scatter_group(jnp.dot(attended, out_use, preferred_element_type=jnp.float32), pair)
    hidden, normed_one, inverse_one = layer_norm(
        layer_input.astype(jnp.float32) + attn_out, norm1_gain, norm1_bias
    )
    hidden_low = hidden.astype(jnp.bfloat16)
    hidden_group = gather_group(hidden_low, pair)
    upper = jnp.dot(hidden_group, w_up, preferred_element_type=jnp.float32)
    active = gelu_exact(upper).astype(jnp.bfloat16)
    ffn_out = scatter_group(jnp.dot(active, w_down, preferred_element_type=jnp.float32), pair)
    result, normed_two, inverse_two = layer_norm(hidden + ffn_out, norm2_gain, norm2_bias)
    grad_result = out_grad.astype(jnp.float32)
    grad_gain2 = jnp.sum(grad_result * normed_two, axis=0)
    grad_bias2 = jnp.sum(grad_result, axis=0)
    grad_second = norm_back(grad_result, normed_two, inverse_two, norm2_gain)
    branch_low = grad_second.astype(jnp.bfloat16)
    branch_group = gather_group(branch_low, pair)
    grad_active = contract_cols(branch_group, w_down)
    grad_upper = (grad_active * gelu_slope(upper)).astype(jnp.bfloat16)
    grad_down = contract_rows(active, branch_group)
    grad_up = contract_rows(hidden_group, grad_upper)
    summed_up, summed_down = lax.psum((grad_up.astype(jnp.bfloat16), grad_down.astype(jnp.bfloat16)), "dp")
    summed_up, summed_down = summed_up.astype(jnp.float32), summed_down.astype(jnp.float32)
    hidden_part = scatter_group(contract_cols(grad_upper, w_up), pair)
    grad_hidden = grad_second + hidden_part
    grad_gain1 = jnp.sum(grad_hidden * normed_one, axis=0)
    grad_bias1 = jnp.sum(grad_hidden, axis=0)
    grad_first = norm_back(grad_hidden, normed_one, inverse_one, norm1_gain)
    attn_low = grad_first.astype(jnp.bfloat16)
    norm_parts = jnp.zeros((16, grad_gain1.shape[0]), jnp.float32)
    norm_parts = norm_parts.at[:4].set(jnp.stack([grad_gain1, grad_bias1, grad_gain2, grad_bias2]))
    norm_sums = lax.psum(norm_parts, ("dp", "tensor"))
    attn_group = gather_group(attn_low, pair)
    grad_mixed = contract_cols(attn_group, out_use).astype(jnp.bfloat16)
    grad_out_w = contract_rows(attended, attn_group)
    grad_mixed_blocks = grad_mixed.reshape(blocks, row_length, local_heads, head_width)

    def attend_back(pack):
        block, row_segments, log_total, grad_block = pack
        queries = block[:, 0]
        keys = block[:, 1]
        values = block[:, 2]
        scores = masked_scores(queries, keys, row_segments, factor)
        probs = jnp.exp(scores - log_total[..., None])
        grad_probs = jnp.einsum(
            "qhd,khd->hqk", grad_block, values, preferred_element_type=jnp.float32
        )
        grad_scores = probs * (grad_probs - jnp.sum(probs * grad_probs, axis=-1, keepdims=True))
        grad_scores = grad_scores.astype(jnp.bfloat16)
        grad_query = (
            jnp.einsum("hqk,khd->qhd", grad_scores, keys, preferred_element_type=jnp.float32)
            * factor
        )
        grad_key = (
            jnp.einsum("hqk,qhd->khd", grad_scores, queries, preferred_element_type=jnp.float32)
            * factor
        )
        grad_value = jnp.einsum(
            "hqk,qhd->khd",
            probs.astype(jnp.bfloat16),
            grad_block,
            preferred_element_type=jnp.float32,
        )
        stacked = jnp.stack([grad_query, grad_key, grad_value], axis=1)
        return stacked.reshape(row_length, 3, local_width).astype(jnp.bfloat16)

    grad_joined = lax.map(
        attend_back, (joined_blocks, segment_blocks, log_totals, grad_mixed_blocks)
    )
    grad_joined = grad_joined.reshape(group_rows, 3, local_width)
    grad_qkv_w = jnp.einsum("td,tsc->dsc", source, grad_joined, preferred_element_type=jnp.float32)
    input_part = scatter_group(
        jnp.einsum("tsc,dsc->td", grad_joined, qkv_use, preferred_element_type=jnp.float32), pair
    )
    grad_input = grad_first + input_part
    late = (grad_qkv_w.astype(jnp.bfloat16), grad_out_w.astype(jnp.bfloat16))
    late, summed_up, summed_down, norm_sums = lax.optimization_barrier(
        (late, summed_up, summed_down, norm_sums)
    )
    summed_qkv, summed_out = lax.psum(late, "dp")
    summed_qkv, summed_out = summed_qkv.astype(jnp.float32), summed_out.astype(jnp.float32)
    summed_gain1, summed_bias1, summed_gain2, summed_bias2 = (
        norm_sums[0], norm_sums[1], norm_sums[2], norm_sums[3]
    )
    return (
        result.astype(jnp.bfloat16),
        grad_input.astype(jnp.bfloat16),
        summed_qkv,
        summed_out,
        summed_up,
        summed_down,
        summed_gain1,
        summed_bias1,
        summed_gain2,
        summed_bias2,
    )


def solution(mesh):
    return jax.shard_map(
        body,
        mesh=mesh,
        in_specs=(
            P(("dp", "tensor"), None),
            P("dp"),
            P(None, None, "tensor"),
            P("tensor", None),
            P(None, "tensor"),
            P("tensor", None),
            P(),
            P(),
            P(),
            P(),
            P(("dp", "tensor"), None),
        ),
        out_specs=(
            P(("dp", "tensor"), None),
            P(("dp", "tensor"), None),
            P(None, None, "tensor"),
            P("tensor", None),
            P(None, "tensor"),
            P("tensor", None),
            P(),
            P(),
            P(),
            P(),
        ),
        check_vma=False,
    )
```

```python
import jax
import jax.numpy as jnp
from jax import lax
from jax.sharding import PartitionSpec as P

HEAD_DIM = 64
ROW_LEN = 512


EPS = 1e-12
NEG_LARGE = -1e30
SQRT_HALF = 0.7071067811865476
INV_ROOT_TWO_PI = 0.3989422804014327


def gelu_exact(values):
    return 0.5 * values * (1.0 + lax.erf(values * SQRT_HALF))


def gelu_slope(values):
    return (
        0.5 * (1.0 + lax.erf(values * SQRT_HALF))
        + values * jnp.exp(-0.5 * values * values) * INV_ROOT_TWO_PI
    )


def layer_norm(values, gain, bias):
    average = jnp.mean(values, axis=-1, keepdims=True)
    centred = values - average
    inverse = lax.rsqrt(jnp.mean(centred * centred, axis=-1, keepdims=True) + EPS)
    normed = centred * inverse
    return (normed * gain + bias, normed, inverse)


def norm_back(grad, normed, inverse, gain):
    scaled = grad * gain
    return inverse * (
        scaled
        - jnp.mean(scaled, axis=-1, keepdims=True)
        - normed * jnp.mean(scaled * normed, axis=-1, keepdims=True)
    )


def masked_scores(queries, keys, row_segments, factor):
    scores = jnp.einsum("qhd,khd->hqk", queries, keys, preferred_element_type=jnp.float32) * factor
    same = row_segments[:, None] == row_segments[None, :]
    return jnp.where(same[None], scores, NEG_LARGE)


def contract_rows(left, right):
    return lax.dot_general(
        left, right, (((0,), (0,)), ((), ())), preferred_element_type=jnp.float32
    )


def contract_cols(left, right):
    return lax.dot_general(
        left, right, (((1,), (1,)), ((), ())), preferred_element_type=jnp.float32
    )


def _pair_swap(values):
    return lax.ppermute(values, "tensor", [(0, 1), (1, 0)])


def gather_group(values, pair):
    if pair:
        return jnp.concatenate([values, _pair_swap(values)], axis=0)
    return lax.all_gather(values, "tensor", axis=0, tiled=True)


def scatter_group(values, pair):
    if pair:
        rows = values.shape[0] // 2
        own = values[:rows].astype(jnp.float32)
        other = _pair_swap(values[rows:].astype(jnp.bfloat16))
        return own + other.astype(jnp.float32)
    return lax.psum_scatter(
        values.astype(jnp.bfloat16), "tensor", scatter_dimension=0, tiled=True
    ).astype(jnp.float32)


def body(
    layer_input,
    segments,
    w_qkv,
    w_out,
    w_up,
    w_down,
    norm1_gain,
    norm1_bias,
    norm2_gain,
    norm2_bias,
    out_grad,
):
    head_width = HEAD_DIM
    row_length = ROW_LEN
    factor = head_width ** (-0.5)
    qkv_use, out_use = (w_qkv, w_out)
    pair = lax.axis_size("tensor") == 2
    source = gather_group(layer_input, pair)
    local_width = qkv_use.shape[2]
    local_heads = local_width // head_width
    group_rows = source.shape[0]
    blocks = group_rows // row_length
    joined = jnp.einsum("td,dsc->tsc", source, qkv_use, preferred_element_type=jnp.float32).astype(
        jnp.bfloat16
    )
    joined_blocks = joined.reshape(blocks, row_length, 3, local_heads, head_width)
    if pair:
        me = lax.axis_index("tensor")
        own_seg = lax.dynamic_slice_in_dim(segments, me * row_length, row_length)
        other_seg = lax.dynamic_slice_in_dim(segments, (1 - me) * row_length, row_length)
        segments = jnp.concatenate([own_seg, other_seg])
    segment_blocks = segments.reshape(blocks, row_length)

    def attend(pack):
        block, row_segments = pack
        scores = masked_scores(block[:, 0], block[:, 1], row_segments, factor)
        top = jnp.max(scores, axis=-1, keepdims=True)
        expo = jnp.exp(scores - top)
        total = jnp.sum(expo, axis=-1, keepdims=True)
        probs = (expo / total).astype(jnp.bfloat16)
        mixed = jnp.einsum("hqk,khd->qhd", probs, block[:, 2], preferred_element_type=jnp.float32)
        return (
            mixed.reshape(row_length, local_width).astype(jnp.bfloat16),
            (top + jnp.log(total))[..., 0],
        )

    attended, log_totals = lax.map(attend, (joined_blocks, segment_blocks))
    attended = attended.reshape(group_rows, local_width)
    attn_out = scatter_group(jnp.dot(attended, out_use, preferred_element_type=jnp.float32), pair)
    hidden, normed_one, inverse_one = layer_norm(
        layer_input.astype(jnp.float32) + attn_out, norm1_gain, norm1_bias
    )
    hidden_low = hidden.astype(jnp.bfloat16)
    hidden_group = gather_group(hidden_low, pair)
    upper = jnp.dot(hidden_group, w_up, preferred_element_type=jnp.float32)
    active = gelu_exact(upper).astype(jnp.bfloat16)
    ffn_out = scatter_group(jnp.dot(active, w_down, preferred_element_type=jnp.float32), pair)
    result, normed_two, inverse_two = layer_norm(hidden + ffn_out, norm2_gain, norm2_bias)
    grad_result = out_grad.astype(jnp.float32)
    grad_gain2 = jnp.sum(grad_result * normed_two, axis=0)
    grad_bias2 = jnp.sum(grad_result, axis=0)
    grad_second = norm_back(grad_result, normed_two, inverse_two, norm2_gain)
    branch_low = grad_second.astype(jnp.bfloat16)
    branch_group = gather_group(branch_low, pair)
    grad_active = contract_cols(branch_group, w_down)
    grad_upper = (grad_active * gelu_slope(upper)).astype(jnp.bfloat16)
    grad_down = contract_rows(active, branch_group)
    grad_up = contract_rows(hidden_group, grad_upper)
    summed_up, summed_down = lax.psum((grad_up.astype(jnp.bfloat16), grad_down.astype(jnp.bfloat16)), "dp")
    summed_up, summed_down = summed_up.astype(jnp.float32), summed_down.astype(jnp.float32)
    hidden_part = scatter_group(contract_cols(grad_upper, w_up), pair)
    grad_hidden = grad_second + hidden_part
    grad_gain1 = jnp.sum(grad_hidden * normed_one, axis=0)
    grad_bias1 = jnp.sum(grad_hidden, axis=0)
    grad_first = norm_back(grad_hidden, normed_one, inverse_one, norm1_gain)
    attn_low = grad_first.astype(jnp.bfloat16)
    attn_group = gather_group(attn_low, pair)
    grad_mixed = contract_cols(attn_group, out_use).astype(jnp.bfloat16)
    grad_out_w = contract_rows(attended, attn_group)
    grad_mixed_blocks = grad_mixed.reshape(blocks, row_length, local_heads, head_width)

    def attend_back(pack):
        block, row_segments, log_total, grad_block = pack
        queries = block[:, 0]
        keys = block[:, 1]
        values = block[:, 2]
        scores = masked_scores(queries, keys, row_segments, factor)
        probs = jnp.exp(scores - log_total[..., None])
        grad_probs = jnp.einsum(
            "qhd,khd->hqk", grad_block, values, preferred_element_type=jnp.float32
        )
        grad_scores = probs * (grad_probs - jnp.sum(probs * grad_probs, axis=-1, keepdims=True))
        grad_scores = grad_scores.astype(jnp.bfloat16)
        grad_query = (
            jnp.einsum("hqk,khd->qhd", grad_scores, keys, preferred_element_type=jnp.float32)
            * factor
        )
        grad_key = (
            jnp.einsum("hqk,qhd->khd", grad_scores, queries, preferred_element_type=jnp.float32)
            * factor
        )
        grad_value = jnp.einsum(
            "hqk,qhd->khd",
            probs.astype(jnp.bfloat16),
            grad_block,
            preferred_element_type=jnp.float32,
        )
        stacked = jnp.stack([grad_query, grad_key, grad_value], axis=1)
        return stacked.reshape(row_length, 3, local_width).astype(jnp.bfloat16)

    grad_joined = lax.map(
        attend_back, (joined_blocks, segment_blocks, log_totals, grad_mixed_blocks)
    )
    grad_joined = grad_joined.reshape(group_rows, 3, local_width)
    grad_qkv_w = jnp.einsum("td,tsc->dsc", source, grad_joined, preferred_element_type=jnp.float32)
    input_part = scatter_group(
        jnp.einsum("tsc,dsc->td", grad_joined, qkv_use, preferred_element_type=jnp.float32), pair
    )
    grad_input = grad_first + input_part
    late = (grad_qkv_w.astype(jnp.bfloat16), grad_out_w.astype(jnp.bfloat16))
    norm_parts = (grad_gain1, grad_bias1, grad_gain2, grad_bias2)
    late, summed_up, summed_down, norm_parts = lax.optimization_barrier(
        (late, summed_up, summed_down, norm_parts)
    )
    summed_qkv, summed_out = lax.psum(late, "dp")
    summed_qkv, summed_out = summed_qkv.astype(jnp.float32), summed_out.astype(jnp.float32)
    summed_gain1, summed_bias1, summed_gain2, summed_bias2 = lax.psum(norm_parts, ("dp", "tensor"))
    return (
        result.astype(jnp.bfloat16),
        grad_input.astype(jnp.bfloat16),
        summed_qkv,
        summed_out,
        summed_up,
        summed_down,
        summed_gain1,
        summed_bias1,
        summed_gain2,
        summed_bias2,
    )


def solution(mesh):
    return jax.shard_map(
        body,
        mesh=mesh,
        in_specs=(
            P(("dp", "tensor"), None),
            P("dp"),
            P(None, None, "tensor"),
            P("tensor", None),
            P(None, "tensor"),
            P("tensor", None),
            P(),
            P(),
            P(),
            P(),
            P(("dp", "tensor"), None),
        ),
        out_specs=(
            P(("dp", "tensor"), None),
            P(("dp", "tensor"), None),
            P(None, None, "tensor"),
            P("tensor", None),
            P(None, "tensor"),
            P("tensor", None),
            P(),
            P(),
            P(),
            P(),
        ),
        check_vma=False,
    )
```

```python
import jax
import jax.numpy as jnp
from jax import lax
from jax.sharding import PartitionSpec as P

HEAD_DIM = 64
ROW_LEN = 512


EPS = 1e-12
NEG_LARGE = -1e30
SQRT_HALF = 0.7071067811865476
INV_ROOT_TWO_PI = 0.3989422804014327


def gelu_exact(values):
    return 0.5 * values * (1.0 + lax.erf(values * SQRT_HALF))


def gelu_slope(values):
    return (
        0.5 * (1.0 + lax.erf(values * SQRT_HALF))
        + values * jnp.exp(-0.5 * values * values) * INV_ROOT_TWO_PI
    )


def layer_norm(values, gain, bias):
    average = jnp.mean(values, axis=-1, keepdims=True)
    centred = values - average
    inverse = lax.rsqrt(jnp.mean(centred * centred, axis=-1, keepdims=True) + EPS)
    normed = centred * inverse
    return (normed * gain + bias, normed, inverse)


def norm_back(grad, normed, inverse, gain):
    scaled = grad * gain
    return inverse * (
        scaled
        - jnp.mean(scaled, axis=-1, keepdims=True)
        - normed * jnp.mean(scaled * normed, axis=-1, keepdims=True)
    )


def masked_scores(queries, keys, row_segments, factor):
    scores = jnp.einsum("qhd,khd->hqk", queries, keys, preferred_element_type=jnp.float32) * factor
    same = row_segments[:, None] == row_segments[None, :]
    return jnp.where(same[None], scores, NEG_LARGE)


def contract_rows(left, right):
    return lax.dot_general(
        left, right, (((0,), (0,)), ((), ())), preferred_element_type=jnp.float32
    )


def contract_cols(left, right):
    return lax.dot_general(
        left, right, (((1,), (1,)), ((), ())), preferred_element_type=jnp.float32
    )


def _pair_swap(values):
    return lax.ppermute(values, "tensor", [(0, 1), (1, 0)])


def gather_group(values, pair):
    if pair:
        return jnp.concatenate([values, _pair_swap(values)], axis=0)
    return lax.all_gather(values, "tensor", axis=0, tiled=True)


def scatter_group(values, pair):
    if pair:
        rows = values.shape[0] // 2
        own = values[:rows].astype(jnp.float32)
        other = _pair_swap(values[rows:].astype(jnp.bfloat16))
        return own + other.astype(jnp.float32)
    return lax.psum_scatter(
        values.astype(jnp.bfloat16), "tensor", scatter_dimension=0, tiled=True
    ).astype(jnp.float32)


def body(
    layer_input,
    segments,
    w_qkv,
    w_out,
    w_up,
    w_down,
    norm1_gain,
    norm1_bias,
    norm2_gain,
    norm2_bias,
    out_grad,
):
    head_width = HEAD_DIM
    row_length = ROW_LEN
    factor = head_width ** (-0.5)
    qkv_use, out_use = (w_qkv, w_out)
    pair = lax.axis_size("tensor") == 2
    source = gather_group(layer_input, pair)
    local_width = qkv_use.shape[2]
    local_heads = local_width // head_width
    group_rows = source.shape[0]
    blocks = group_rows // row_length
    joined = jnp.einsum("td,dsc->tsc", source, qkv_use, preferred_element_type=jnp.float32).astype(
        jnp.bfloat16
    )
    joined_blocks = joined.reshape(blocks, row_length, 3, local_heads, head_width)
    if pair:
        me = lax.axis_index("tensor")
        own_seg = lax.dynamic_slice_in_dim(segments, me * row_length, row_length)
        other_seg = lax.dynamic_slice_in_dim(segments, (1 - me) * row_length, row_length)
        segments = jnp.concatenate([own_seg, other_seg])
    segment_blocks = segments.reshape(blocks, row_length)

    def attend(pack):
        block, row_segments = pack
        scores = masked_scores(block[:, 0], block[:, 1], row_segments, factor)
        top = jnp.max(scores, axis=-1, keepdims=True)
        expo = jnp.exp(scores - top)
        total = jnp.sum(expo, axis=-1, keepdims=True)
        probs = (expo / total).astype(jnp.bfloat16)
        mixed = jnp.einsum("hqk,khd->qhd", probs, block[:, 2], preferred_element_type=jnp.float32)
        return (
            mixed.reshape(row_length, local_width).astype(jnp.bfloat16),
            (top + jnp.log(total))[..., 0],
        )

    attended, log_totals = lax.map(attend, (joined_blocks, segment_blocks))
    attended = attended.reshape(group_rows, local_width)
    attn_out = scatter_group(jnp.dot(attended, out_use, preferred_element_type=jnp.float32), pair)
    hidden, normed_one, inverse_one = layer_norm(
        layer_input.astype(jnp.float32) + attn_out, norm1_gain, norm1_bias
    )
    hidden_low = hidden.astype(jnp.bfloat16)
    hidden_group = gather_group(hidden_low, pair)
    upper = jnp.dot(hidden_group, w_up, preferred_element_type=jnp.float32)
    active = gelu_exact(upper).astype(jnp.bfloat16)
    ffn_out = scatter_group(jnp.dot(active, w_down, preferred_element_type=jnp.float32), pair)
    result, normed_two, inverse_two = layer_norm(hidden + ffn_out, norm2_gain, norm2_bias)
    grad_result = out_grad.astype(jnp.float32)
    grad_gain2 = jnp.sum(grad_result * normed_two, axis=0)
    grad_bias2 = jnp.sum(grad_result, axis=0)
    grad_second = norm_back(grad_result, normed_two, inverse_two, norm2_gain)
    branch_low = grad_second.astype(jnp.bfloat16)
    branch_group = gather_group(branch_low, pair)
    grad_active = contract_cols(branch_group, w_down)
    grad_upper = (grad_active * gelu_slope(upper)).astype(jnp.bfloat16)
    grad_down = contract_rows(active, branch_group)
    grad_up = contract_rows(hidden_group, grad_upper)
    summed_up, summed_down = lax.psum((grad_up.astype(jnp.bfloat16), grad_down.astype(jnp.bfloat16)), "dp")
    summed_up, summed_down = summed_up.astype(jnp.float32), summed_down.astype(jnp.float32)
    hidden_part = scatter_group(contract_cols(grad_upper, w_up), pair)
    grad_hidden = grad_second + hidden_part
    grad_gain1 = jnp.sum(grad_hidden * normed_one, axis=0)
    grad_bias1 = jnp.sum(grad_hidden, axis=0)
    grad_first = norm_back(grad_hidden, normed_one, inverse_one, norm1_gain)
    attn_low = grad_first.astype(jnp.bfloat16)
    attn_group = gather_group(attn_low, pair)
    grad_mixed = contract_cols(attn_group, out_use).astype(jnp.bfloat16)
    grad_out_w = contract_rows(attended, attn_group)
    grad_mixed_blocks = grad_mixed.reshape(blocks, row_length, local_heads, head_width)

    def attend_back(pack):
        block, row_segments, log_total, grad_block = pack
        queries = block[:, 0]
        keys = block[:, 1]
        values = block[:, 2]
        scores = masked_scores(queries, keys, row_segments, factor)
        probs = jnp.exp(scores - log_total[..., None])
        grad_probs = jnp.einsum(
            "qhd,khd->hqk", grad_block, values, preferred_element_type=jnp.float32
        )
        grad_scores = probs * (grad_probs - jnp.sum(probs * grad_probs, axis=-1, keepdims=True))
        grad_scores = grad_scores.astype(jnp.bfloat16)
        grad_query = (
            jnp.einsum("hqk,khd->qhd", grad_scores, keys, preferred_element_type=jnp.float32)
            * factor
        )
        grad_key = (
            jnp.einsum("hqk,qhd->khd", grad_scores, queries, preferred_element_type=jnp.float32)
            * factor
        )
        grad_value = jnp.einsum(
            "hqk,qhd->khd",
            probs.astype(jnp.bfloat16),
            grad_block,
            preferred_element_type=jnp.float32,
        )
        stacked = jnp.stack([grad_query, grad_key, grad_value], axis=1)
        return stacked.reshape(row_length, 3, local_width).astype(jnp.bfloat16)

    grad_joined = lax.map(
        attend_back, (joined_blocks, segment_blocks, log_totals, grad_mixed_blocks)
    )
    grad_joined = grad_joined.reshape(group_rows, 3, local_width)
    grad_qkv_w = jnp.einsum("td,tsc->dsc", source, grad_joined, preferred_element_type=jnp.float32)
    input_part = scatter_group(
        jnp.einsum("tsc,dsc->td", grad_joined, qkv_use, preferred_element_type=jnp.float32), pair
    )
    grad_input = grad_first + input_part
    late = (grad_qkv_w.astype(jnp.bfloat16), grad_out_w.astype(jnp.bfloat16))
    norm_parts = (grad_gain1, grad_bias1, grad_gain2, grad_bias2)
    late, summed_up, summed_down, norm_parts = lax.optimization_barrier(
        (late, summed_up, summed_down, norm_parts)
    )
    summed_qkv, summed_out = lax.psum(late, "dp")
    summed_qkv, summed_out = summed_qkv.astype(jnp.float32), summed_out.astype(jnp.float32)
    summed_gain1, summed_bias1, summed_gain2, summed_bias2 = lax.psum(norm_parts, ("dp", "tensor"))
    return (
        result.astype(jnp.bfloat16),
        grad_input.astype(jnp.bfloat16),
        summed_qkv,
        summed_out,
        summed_up,
        summed_down,
        summed_gain1,
        summed_bias1,
        summed_gain2,
        summed_bias2,
    )


def attend_row(qkv, row_segments, factor):
    rows, _, width = qkv.shape
    heads = width // HEAD_DIM
    block = qkv.reshape(rows, 3, heads, HEAD_DIM)
    scores = masked_scores(block[:, 0], block[:, 1], row_segments, factor)
    top = jnp.max(scores, axis=-1, keepdims=True)
    expo = jnp.exp(scores - top)
    total = jnp.sum(expo, axis=-1, keepdims=True)
    probs = (expo / total).astype(jnp.bfloat16)
    mixed = jnp.einsum("hqk,khd->qhd", probs, block[:, 2], preferred_element_type=jnp.float32)
    return mixed.reshape(rows, width).astype(jnp.bfloat16), (top + jnp.log(total))[..., 0]


def attend_row_back(qkv, row_segments, log_total, grad_mixed, factor):
    rows, _, width = qkv.shape
    heads = width // HEAD_DIM
    block = qkv.reshape(rows, 3, heads, HEAD_DIM)
    queries = block[:, 0]
    keys = block[:, 1]
    values = block[:, 2]
    grad_block = grad_mixed.reshape(rows, heads, HEAD_DIM)
    scores = masked_scores(queries, keys, row_segments, factor)
    probs = jnp.exp(scores - log_total[..., None])
    grad_probs = jnp.einsum("qhd,khd->hqk", grad_block, values, preferred_element_type=jnp.float32)
    grad_scores = probs * (grad_probs - jnp.sum(probs * grad_probs, axis=-1, keepdims=True))
    grad_scores = grad_scores.astype(jnp.bfloat16)
    grad_query = (
        jnp.einsum("hqk,khd->qhd", grad_scores, keys, preferred_element_type=jnp.float32) * factor
    )
    grad_key = (
        jnp.einsum("hqk,qhd->khd", grad_scores, queries, preferred_element_type=jnp.float32) * factor
    )
    grad_value = jnp.einsum(
        "hqk,qhd->khd", probs.astype(jnp.bfloat16), grad_block, preferred_element_type=jnp.float32
    )
    stacked = jnp.stack([grad_query, grad_key, grad_value], axis=1)
    return stacked.reshape(rows, 3, width).astype(jnp.bfloat16)


def body_pair(
    layer_input,
    segments,
    w_qkv,
    w_out,
    w_up,
    w_down,
    norm1_gain,
    norm1_bias,
    norm2_gain,
    norm2_bias,
    out_grad,
):
    factor = HEAD_DIM ** (-0.5)
    rows = layer_input.shape[0]
    me = lax.axis_index("tensor")
    seg_o = lax.dynamic_slice_in_dim(segments, me * rows, rows)
    seg_x = lax.dynamic_slice_in_dim(segments, (1 - me) * rows, rows)

    def project(values):
        return jnp.einsum("td,dsc->tsc", values, w_qkv, preferred_element_type=jnp.float32).astype(
            jnp.bfloat16
        )

    in_x = _pair_swap(layer_input)
    qkv_o = project(layer_input)
    qkv_x = project(in_x)
    att_x, lse_x = attend_row(qkv_x, seg_x, factor)
    part_x = jnp.dot(att_x, w_out, preferred_element_type=jnp.float32)
    recv = _pair_swap(part_x.astype(jnp.bfloat16))
    att_o, lse_o = attend_row(qkv_o, seg_o, factor)
    part_o = jnp.dot(att_o, w_out, preferred_element_type=jnp.float32)
    attn_out = part_o + recv.astype(jnp.float32)
    hidden, normed_one, inverse_one = layer_norm(
        layer_input.astype(jnp.float32) + attn_out, norm1_gain, norm1_bias
    )
    hid_o = hidden.astype(jnp.bfloat16)

    hid_x = _pair_swap(hid_o)
    up_o = jnp.dot(hid_o, w_up, preferred_element_type=jnp.float32)
    act_o = gelu_exact(up_o).astype(jnp.bfloat16)
    up_x = jnp.dot(hid_x, w_up, preferred_element_type=jnp.float32)
    act_x = gelu_exact(up_x).astype(jnp.bfloat16)
    down_x = jnp.dot(act_x, w_down, preferred_element_type=jnp.float32)
    recv = _pair_swap(down_x.astype(jnp.bfloat16))
    down_o = jnp.dot(act_o, w_down, preferred_element_type=jnp.float32)
    ffn_out = down_o + recv.astype(jnp.float32)
    result, normed_two, inverse_two = layer_norm(hidden + ffn_out, norm2_gain, norm2_bias)

    grad_result = out_grad.astype(jnp.float32)
    grad_gain2 = jnp.sum(grad_result * normed_two, axis=0)
    grad_bias2 = jnp.sum(grad_result, axis=0)
    grad_second = norm_back(grad_result, normed_two, inverse_two, norm2_gain)
    br_o = grad_second.astype(jnp.bfloat16)

    br_x = _pair_swap(br_o)
    gu_o = (contract_cols(br_o, w_down) * gelu_slope(up_o)).astype(jnp.bfloat16)
    gu_x = (contract_cols(br_x, w_down) * gelu_slope(up_x)).astype(jnp.bfloat16)
    hp_x = contract_cols(gu_x, w_up)
    recv = _pair_swap(hp_x.astype(jnp.bfloat16))
    grad_down = contract_rows(act_o, br_o) + contract_rows(act_x, br_x)
    grad_up = contract_rows(hid_o, gu_o) + contract_rows(hid_x, gu_x)
    summed_up, summed_down = lax.psum(
        (grad_up.astype(jnp.bfloat16), grad_down.astype(jnp.bfloat16)), "dp"
    )
    summed_up, summed_down = summed_up.astype(jnp.float32), summed_down.astype(jnp.float32)
    hp_o = contract_cols(gu_o, w_up)
    grad_hidden = grad_second + hp_o + recv.astype(jnp.float32)

    grad_gain1 = jnp.sum(grad_hidden * normed_one, axis=0)
    grad_bias1 = jnp.sum(grad_hidden, axis=0)
    grad_first = norm_back(grad_hidden, normed_one, inverse_one, norm1_gain)
    da_o = grad_first.astype(jnp.bfloat16)

    da_x = _pair_swap(da_o)
    gm_o = contract_cols(da_o, w_out).astype(jnp.bfloat16)
    gj_o = attend_row_back(qkv_o, seg_o, lse_o, gm_o, factor)
    gm_x = contract_cols(da_x, w_out).astype(jnp.bfloat16)
    gj_x = attend_row_back(qkv_x, seg_x, lse_x, gm_x, factor)

    def back_project(values):
        return jnp.einsum("tsc,dsc->td", values, w_qkv, preferred_element_type=jnp.float32)

    ip_x = back_project(gj_x)
    recv = _pair_swap(ip_x.astype(jnp.bfloat16))
    grad_out_w = contract_rows(att_o, da_o) + contract_rows(att_x, da_x)
    grad_qkv_w = jnp.einsum(
        "td,tsc->dsc", layer_input, gj_o, preferred_element_type=jnp.float32
    ) + jnp.einsum("td,tsc->dsc", in_x, gj_x, preferred_element_type=jnp.float32)
    ip_o = back_project(gj_o)
    grad_input = grad_first + ip_o + recv.astype(jnp.float32)

    late = (grad_qkv_w.astype(jnp.bfloat16), grad_out_w.astype(jnp.bfloat16))
    norm_parts = (grad_gain1, grad_bias1, grad_gain2, grad_bias2)
    late, summed_up, summed_down, norm_parts = lax.optimization_barrier(
        (late, summed_up, summed_down, norm_parts)
    )
    summed_qkv, summed_out = lax.psum(late, "dp")
    summed_qkv, summed_out = summed_qkv.astype(jnp.float32), summed_out.astype(jnp.float32)
    summed_gain1, summed_bias1, summed_gain2, summed_bias2 = lax.psum(norm_parts, ("dp", "tensor"))
    return (
        result.astype(jnp.bfloat16),
        grad_input.astype(jnp.bfloat16),
        summed_qkv,
        summed_out,
        summed_up,
        summed_down,
        summed_gain1,
        summed_bias1,
        summed_gain2,
        summed_bias2,
    )


def solution(mesh):
    return jax.shard_map(
        body_pair if mesh.shape["tensor"] == 2 else body,
        mesh=mesh,
        in_specs=(
            P(("dp", "tensor"), None),
            P("dp"),
            P(None, None, "tensor"),
            P("tensor", None),
            P(None, "tensor"),
            P("tensor", None),
            P(),
            P(),
            P(),
            P(),
            P(("dp", "tensor"), None),
        ),
        out_specs=(
            P(("dp", "tensor"), None),
            P(("dp", "tensor"), None),
            P(None, None, "tensor"),
            P("tensor", None),
            P(None, "tensor"),
            P("tensor", None),
            P(),
            P(),
            P(),
            P(),
        ),
        check_vma=False,
    )
```
